32 devices in a mesh: replica: 2 (over x), data2: 4 (over z), data: 4 (over y, core).
Axes of the slice: x: 2, y: 2, z: 4, core: 2. Of those that a mesh axis runs over, the one named last changes fastest.
Arguments:
- query_hidden: bfloat16 [256, 32, 768], P(('replica', 'data2', 'data')), parts along dimension 0
- doc_hidden: bfloat16 [256, 300, 768], P(('replica', 'data2', 'data')), parts along dimension 0
- w_proj: bfloat16 [768, 128], replicated
- query_mask: int32 [256, 32], P(('replica', 'data2', 'data')), parts along dimension 0
- doc_mask: int32 [256, 300], P(('replica', 'data2', 'data')), parts along dimension 0
- temperature: float32 [], replicated
Outputs:
- output 1: float32 [256], P(('replica', 'data2', 'data')), parts along dimension 0
- output 2: float32 [2], P('replica'), parts along dimension 0
There are 2 independent parts. The reference program is written for one: setup_inputs(seed, part) draws one part's arguments, and reference() takes and returns one part's arrays. A program takes and returns all parts, laid end to end along the dimension named above; an argument that names none is the same for every part.
All inputs are finite; a program needn't handle non-finite values.
Results may differ from the reference program's by a relative error of at most 0.001.
Values are sent between devices in bfloat16 or wider.
A program may use at most 1 GiB of HBM per device.

```python
import jax
import jax.numpy as jnp
from jax import lax

BATCH = 128
QLEN = 32
DLEN = 300
HIDDEN = 768
PROJ = 128


def setup_inputs(seed: int = 0, part: int = 0) -> dict:
    root_key = jax.random.key(seed)
    key_common, key_parts = jax.random.split(root_key)
    part_key = jax.random.fold_in(key_parts, part)
    key_list = jax.random.split(part_key, 6)
    key_weight, key_temp = jax.random.split(key_common)
    shared = jax.random.normal(key_list[0], (HIDDEN,), jnp.float32)
    topic_vec = jax.random.normal(key_list[1], (BATCH, 1, HIDDEN), jnp.float32)
    concept = jax.random.normal(key_list[2], (BATCH, QLEN, HIDDEN), jnp.float32)
    token_noise = jax.random.normal(key_list[3], (BATCH, DLEN, HIDDEN), jnp.float32)
    query_lens = jax.random.randint(key_list[4], (BATCH,), QLEN // 2, QLEN + 1)
    doc_lens = jax.random.randint(key_list[5], (BATCH,), DLEN // 4, DLEN + 1)
    query_mask = (jnp.arange(QLEN)[None, :] < query_lens[:, None]).astype(jnp.int32)
    doc_mask = (jnp.arange(DLEN)[None, :] < doc_lens[:, None]).astype(jnp.int32)
    base_state = 0.6 * shared + 0.6 * topic_vec
    query_hidden = base_state + concept
    doc_concept = jnp.take(concept, jnp.arange(DLEN) % QLEN, axis=1)
    real_tok = base_state + 0.6 * doc_concept + 0.8 * token_noise
    pad_tok = 1.5 * shared + token_noise
    doc_hidden = jnp.where(doc_mask[:, :, None] > 0, real_tok, pad_tok)
    w_proj = jax.random.normal(key_weight, (HIDDEN, PROJ), jnp.float32) * HIDDEN ** -0.5
    temperature = QLEN * jax.random.uniform(key_temp, (), jnp.float32, 0.8, 1.25) / 8.0
    return {'query_hidden': query_hidden.astype(jnp.bfloat16), 'doc_hidden': doc_hidden.astype(jnp.bfloat16), 'w_proj': w_proj.astype(jnp.bfloat16), 'query_mask': query_mask, 'doc_mask': doc_mask, 'temperature': temperature}


def project_norm(hidden, w_proj):
    flat_states = hidden.reshape(-1, HIDDEN)
    projected = jnp.dot(flat_states, w_proj, preferred_element_type=jnp.float32)
    norm_len = jnp.sqrt(jnp.sum(projected * projected, axis=-1, keepdims=True))
    unit_vecs = projected / jnp.maximum(norm_len, 1e-12)
    return unit_vecs.astype(jnp.bfloat16).reshape(hidden.shape[0], hidden.shape[1], PROJ)


def reference(query_hidden, doc_hidden, w_proj, query_mask, doc_mask, temperature):
    q_vecs = project_norm(query_hidden, w_proj)
    p_vecs = project_norm(doc_hidden, w_proj).astype(jnp.float32)
    doc_valid = doc_mask[None, :, :] > 0

    def query_row(query_args):
        q_tok, q_weight = query_args
        similarity = jnp.einsum('tc,jsc->tjs', q_tok.astype(jnp.float32), p_vecs)
        best_match = jnp.max(jnp.where(doc_valid, similarity, -jnp.inf), axis=-1)
        return jnp.sum(q_weight.astype(jnp.float32)[:, None] * best_match, axis=0)

    scores = lax.map(query_row, (q_vecs, query_mask))
    logits = scores / temperature
    losses = jax.nn.logsumexp(logits, axis=1) - jnp.diagonal(logits)
    mean_loss = jnp.mean(losses).reshape(1)
    return losses, mean_loss
```

```python
import functools

import jax
import jax.numpy as jnp
from jax import lax
from jax.experimental import pallas as pl
from jax.experimental.pallas import tpu as pltpu
from jax.sharding import PartitionSpec as P

F32 = jnp.float32
BF16 = jnp.bfloat16
LANES = 128
BIG = 1e30


def inv_norm(x, axis):
    return lax.rsqrt(jnp.maximum(jnp.sum(x * x, axis=axis, keepdims=True), 1e-24))


def iota(shape, dim):
    return lax.broadcasted_iota(jnp.int32, shape, dim)


def kernel(dims, q_hbm, d_hbm, w_hbm, qm_hbm, dm_hbm, t_hbm, loss_ref, mean_ref,
           qh, dh, w, qm, dm, temp, dmp, pa, qb, bm, st,
           in_sem, doc_sem, send_sem, recv_sem, ssend_sem, srecv_sem):
    nz, ny, nb, qlen, dlen, drow, hidden = dims
    group = nz * ny * 2
    qtok = nb * qlen
    z = lax.axis_index('data2')
    yc = lax.axis_index('data')
    y = yc // 2
    c = yc % 2
    me = z * (2 * ny) + yc

    def dev(zz, yy, cc):
        return {'data2': zz, 'data': yy * 2 + cc}

    def bid(zz, yy, cc):
        return zz * (2 * ny) + yy * 2 + cc

    oy, oc = 1 - y, 1 - c
    zx = (z + 1 - 2 * (z % 2), (z + 2) % 4, 3 - z)

    loads = [
        pltpu.make_async_copy(qm_hbm, qm, in_sem.at[0]),
        pltpu.make_async_copy(w_hbm, w, in_sem.at[1]),
        pltpu.make_async_copy(q_hbm, qh, in_sem.at[2]),
        pltpu.make_async_copy(dm_hbm, dm, in_sem.at[3]),
        pltpu.make_async_copy(t_hbm, temp, in_sem.at[4]),
    ]
    for cp in loads:
        cp.start()
    docs = [pltpu.make_async_copy(d_hbm.at[j], dh.at[j], doc_sem.at[j]) for j in range(nb)]
    for cp in docs:
        cp.start()

    barrier = pltpu.get_barrier_semaphore()
    near = [dev(z, y, oc), dev(z, oy, c)] + [dev(k, y, c) for k in zx]
    for d in near:
        pl.semaphore_signal(barrier, inc=1, device_id=d, device_id_type=pl.DeviceIdType.MESH)

    loads[0].wait()
    spread = (iota((qlen, qtok), 1) % qlen == iota((qlen, qtok), 0)).astype(BF16)
    qmf = jnp.dot(qm[...].astype(F32).astype(BF16), spread, preferred_element_type=F32)
    own_row = iota((nb, qtok), 1) // qlen == iota((nb, qtok), 0)
    qmask = jnp.sum(jnp.where(own_row, qmf, 0.0), axis=0, keepdims=True)
    loads[1].wait()
    loads[2].wait()
    qp = jnp.dot(qh[...].reshape(qtok, hidden), w[...], preferred_element_type=F32)
    qt = qp.T
    qt = qt * inv_norm(qt, 0)
    qb[me] = jnp.where(qmask > 0, qt, 0.0).astype(BF16)

    pl.semaphore_wait(barrier, len(near))

    sends = []

    def send(block, d):
        k = len(sends)
        cp = pltpu.make_async_remote_copy(
            src_ref=qb.at[block], dst_ref=qb.at[block], send_sem=send_sem.at[k],
            recv_sem=recv_sem.at[block], device_id=d, device_id_type=pl.DeviceIdType.MESH)
        cp.start()
        sends.append(cp)

    def arrive(block):
        pltpu.make_async_remote_copy(
            src_ref=qb.at[block], dst_ref=qb.at[block], send_sem=send_sem.at[0],
            recv_sem=recv_sem.at[block], device_id=dev(z, y, oc),
            device_id_type=pl.DeviceIdType.MESH).wait_recv()

    to_core, to_y = dev(z, y, oc), dev(z, oy, c)
    for k in zx:
        send(me, dev(k, y, c))
    send(me, to_y)
    send(me, to_core)

    loads[3].wait()
    dmp[...] = jnp.full(dmp.shape, -1.0, F32)
    dmp[:, pl.ds(0, dlen)] = dm[...].astype(F32) - 1.0
    pick = jnp.where(iota((nb, nb * LANES), 1) == iota((nb, nb * LANES), 0) * LANES, BIG, 0.0)
    bias = lax.dot_general(dmp[...], pick, (((0,), (0,)), ((), ())), preferred_element_type=F32)
    for j in range(nb):
        pa[pl.ds(j * drow, drow), pl.ds(LANES, LANES)] = (
            bias[:drow, j * LANES:(j + 1) * LANES].astype(BF16))
    for j in range(nb):
        pa[pl.ds((j + 1) * drow - 16, 16), pl.ds(0, LANES)] = jnp.zeros((16, LANES), BF16)
        docs[j].wait()
        dp = jnp.dot(dh[j], w[...], preferred_element_type=F32)
        pa[pl.ds(j * drow, dlen), pl.ds(0, LANES)] = (dp * inv_norm(dp, 1)).astype(BF16)

    ones_row = (iota((LANES, qtok), 0) == 0).astype(BF16)

    def score(block):
        rhs = jnp.concatenate([qb[block], ones_row], axis=0)
        sim = jnp.dot(pa[...], rhs, preferred_element_type=F32)
        bm[block] = jnp.max(sim.reshape(nb, drow, qtok), axis=1)

    def step(block, fwd=()):
        arrive(block)
        for d in fwd:
            send(block, d)
        score(block)

    score(me)
    step(bid(z, y, oc))
    step(bid(z, oy, c), (to_core,))
    step(bid(zx[0], y, c), (to_y, to_core))
    step(bid(z, oy, oc))
    step(bid(zx[1], y, c), (to_y, to_core))
    step(bid(zx[0], y, oc))
    step(bid(zx[0], oy, c), (to_core,))
    step(bid(zx[2], y, c), (to_y, to_core))
    step(bid(zx[1], y, oc))
    step(bid(zx[1], oy, c), (to_core,))
    step(bid(zx[0], oy, oc))
    step(bid(zx[2], y, oc))
    step(bid(zx[2], oy, c), (to_core,))
    step(bid(zx[1], oy, oc))
    step(bid(zx[2], oy, oc))

    best = bm[...].reshape(group * nb, qtok)
    sel = (iota((qtok, LANES), 0) // qlen == iota((qtok, LANES), 1) % nb).astype(BF16)
    hi = best.astype(BF16)
    rest = best - hi.astype(F32)
    mid = rest.astype(BF16)
    low = (rest - mid.astype(F32)).astype(BF16)
    tot = (jnp.dot(low, sel, preferred_element_type=F32)
           + jnp.dot(mid, sel, preferred_element_type=F32)
           + jnp.dot(hi, sel, preferred_element_type=F32))
    tot = tot.reshape(group, nb, LANES)
    here = iota((group, nb, LANES), 2) // nb == iota((group, nb, LANES), 0)
    scores = jnp.sum(jnp.where(here, tot, 0.0), axis=0)

    loads[4].wait()
    logits = scores / temp[0]
    top = jnp.max(logits, axis=0, keepdims=True)
    part = jnp.sum(jnp.exp(logits - top), axis=0, keepdims=True)
    mine = iota((nb, LANES), 1) == me * nb + iota((nb, LANES), 0)
    diag = jnp.sum(jnp.where(mine, logits, 0.0), axis=0, keepdims=True)
    st[me] = jnp.concatenate([top, part, diag, jnp.zeros_like(diag)], axis=0)

    stats = []
    for k in range(1, group):
        peer = (me + k) % group
        cp = pltpu.make_async_remote_copy(
            src_ref=st.at[me], dst_ref=st.at[me], send_sem=ssend_sem.at[k],
            recv_sem=srecv_sem.at[me],
            device_id={'data2': peer // (2 * ny), 'data': peer % (2 * ny)},
            device_id_type=pl.DeviceIdType.MESH)
        cp.start()
        stats.append(cp)
    for k in range(1, group):
        peer = (me + k) % group
        pltpu.make_async_remote_copy(
            src_ref=st.at[peer], dst_ref=st.at[peer], send_sem=ssend_sem.at[0],
            recv_sem=srecv_sem.at[peer], device_id=dev(z, y, oc),
            device_id_type=pl.DeviceIdType.MESH).wait_recv()

    tops = st[:, 0, :]
    best_top = jnp.max(tops, axis=0, keepdims=True)
    total = jnp.sum(st[:, 1, :] * jnp.exp(tops - best_top), axis=0, keepdims=True)
    losses = best_top + jnp.log(total) - jnp.sum(st[:, 2, :], axis=0, keepdims=True)
    mean_ref[...] = jnp.sum(losses, axis=1, keepdims=True) / (group * nb)
    moved = pltpu.roll(jnp.broadcast_to(losses, (8, LANES)), (LANES - me * nb) % LANES, 1)
    loss_ref[...] = moved[0:1, 0:nb]
    for cp in sends:
        cp.wait_send()
    for cp in stats:
        cp.wait_send()


def solution(mesh):
    nz, nd = mesh.shape['data2'], mesh.shape['data']
    ny = nd // 2
    group = nz * nd
    row_spec = P(('replica', 'data2', 'data'))
    tok_spec = P(('replica', 'data2', 'data'), None, None)
    mask_spec = P(('replica', 'data2', 'data'), None)

    def local_step(qh, dh, w, qm, dm, temp):
        nb, qlen, hidden = qh.shape
        dlen = dh.shape[1]
        drow = -(-dlen // 16) * 16
        dpad = -(-dlen // LANES) * LANES
        dims = (nz, ny, nb, qlen, dlen, drow, hidden)
        losses, mean = pl.pallas_call(
            functools.partial(kernel, dims),
            out_shape=(jax.ShapeDtypeStruct((1, nb), F32), jax.ShapeDtypeStruct((1, 1), F32)),
            in_specs=[pl.BlockSpec(memory_space=pl.ANY)] * 6,
            out_specs=(pl.BlockSpec(memory_space=pltpu.VMEM), pl.BlockSpec(memory_space=pltpu.VMEM)),
            scratch_shapes=[
                pltpu.VMEM((nb, qlen, hidden), BF16),
                pltpu.VMEM((nb, dlen, hidden), BF16),
                pltpu.VMEM(w.shape, BF16),
                pltpu.VMEM((nb, qlen), jnp.int32),
                pltpu.VMEM((nb, dlen), jnp.int32),
                pltpu.SMEM((1,), F32),
                pltpu.VMEM((nb, dpad), F32),
                pltpu.VMEM((nb * drow, 2 * LANES), BF16),
                pltpu.VMEM((group, LANES, nb * qlen), BF16),
                pltpu.VMEM((group, nb, nb * qlen), F32),
                pltpu.VMEM((group, 4, LANES), F32),
                pltpu.SemaphoreType.DMA((5,)),
                pltpu.SemaphoreType.DMA((nb,)),
                pltpu.SemaphoreType.DMA((group,)),
                pltpu.SemaphoreType.DMA((group,)),
                pltpu.SemaphoreType.DMA((group,)),
                pltpu.SemaphoreType.DMA((group,)),
            ],
            compiler_params=pltpu.CompilerParams(collective_id=0, has_side_effects=True),
            name='late_interaction',
        )(qh, dh, w, qm, dm, temp.reshape(1))
        return losses.reshape(nb), mean.reshape(1)

    return jax.shard_map(
        local_step, mesh=mesh,
        in_specs=(tok_spec, tok_spec, P(None, None), mask_spec, mask_spec, P()),
        out_specs=(row_spec, P('replica')), check_vma=False)
```

```python
import functools

import jax
import jax.numpy as jnp
from jax import lax
from jax.experimental import pallas as pl
from jax.experimental.pallas import tpu as pltpu
from jax.sharding import PartitionSpec as P

F32 = jnp.float32
BF16 = jnp.bfloat16
LANES = 128
BIG = 1e30


def inv_norm(x, axis):
    return lax.rsqrt(jnp.maximum(jnp.sum(x * x, axis=axis, keepdims=True), 1e-24))


def iota(shape, dim):
    return lax.broadcasted_iota(jnp.int32, shape, dim)


def kernel(dims, q_hbm, d_hbm, w_hbm, qm_hbm, dm_hbm, t_hbm, out_ref,
           qh, dh, w, qm, dm, temp, pa, qb, bm, st,
           in_sem, doc_sem, send_sem, recv_sem, ssend_sem, srecv_sem):
    nz, ny, nb, qlen, dlen, parts, halves, hidden = dims
    part = dlen * nb // parts
    group = nz * ny * 2
    qtok = nb * qlen
    z = lax.axis_index('data2')
    yc = lax.axis_index('data')
    y = yc // 2
    c = yc % 2
    me = z * (2 * ny) + yc

    def dev(zz, yy, cc):
        return {'data2': zz, 'data': yy * 2 + cc}

    def bid(zz, yy, cc):
        return zz * (2 * ny) + yy * 2 + cc

    oy, oc = 1 - y, 1 - c
    zx = (z + 1 - 2 * (z % 2), (z + 2) % 4, 3 - z)

    loads = [
        pltpu.make_async_copy(qm_hbm, qm, in_sem.at[0]),
        pltpu.make_async_copy(w_hbm, w, in_sem.at[1]),
        pltpu.make_async_copy(q_hbm, qh, in_sem.at[2]),
        pltpu.make_async_copy(dm_hbm, dm, in_sem.at[3]),
        pltpu.make_async_copy(t_hbm, temp, in_sem.at[4]),
    ]
    for cp in loads:
        cp.start()
    docs = [pltpu.make_async_copy(d_hbm.at[pl.ds(j * part, part)], dh.at[pl.ds(j * part, part)],
                                  doc_sem.at[j]) for j in range(parts)]
    for cp in docs:
        cp.start()

    barrier = pltpu.get_barrier_semaphore()
    near = [dev(z, y, oc), dev(z, oy, c)] + [dev(k, y, c) for k in zx]
    for d in near:
        pl.semaphore_signal(barrier, inc=1, device_id=d, device_id_type=pl.DeviceIdType.MESH)

    loads[0].wait()
    spread = (iota((qlen, qtok), 1) % qlen == iota((qlen, qtok), 0)).astype(BF16)
    qmf = jnp.dot(qm[...].astype(F32).astype(BF16), spread, preferred_element_type=F32)
    own_row = iota((nb, qtok), 1) // qlen == iota((nb, qtok), 0)
    qmask = jnp.sum(jnp.where(own_row, qmf, 0.0), axis=0, keepdims=True)
    loads[1].wait()
    loads[2].wait()
    qp = jnp.dot(qh[...].reshape(qtok, hidden), w[...], preferred_element_type=F32)
    qt = qp.T
    qt = qt * inv_norm(qt, 0)
    qb[me] = jnp.where(qmask > 0, qt, 0.0).astype(BF16)

    pl.semaphore_wait(barrier, len(near))

    sends = []
    piece = LANES // halves

    def move(block, h, d, k):
        view = qb.at[block, pl.ds(h * piece, piece)]
        return pltpu.make_async_remote_copy(
            src_ref=view, dst_ref=view, send_sem=send_sem.at[k], recv_sem=recv_sem.at[block, h],
            device_id=d, device_id_type=pl.DeviceIdType.MESH)

    def send(block, h, d):
        cp = move(block, h, d, len(sends))
        cp.start()
        sends.append(cp)

    def arrive(block, fwd=()):
        for h in range(halves):
            move(block, h, to_core, 0).wait_recv()
            for d in fwd:
                send(block, h, d)

    to_core, to_y = dev(z, y, oc), dev(z, oy, c)
    for d in [dev(zx[0], y, c), to_y, dev(zx[1], y, c), dev(zx[2], y, c), to_core]:
        for h in range(halves):
            send(me, h, d)

    loads[3].wait()
    for cp in docs:
        cp.wait()
    bias = (dm[...].astype(F32) - 1.0) * BIG
    for j in range(parts):
        rows = pl.ds(j * part, part)
        dp = jnp.dot(dh[rows], w[...], preferred_element_type=F32)
        pa[rows, pl.ds(0, LANES)] = (dp * inv_norm(dp, 1)).astype(BF16)
        for s in range(j * part // nb, (j + 1) * part // nb, 2):
            pair = [jnp.broadcast_to(bias[:, k:k + 1], (nb, LANES)) for k in (s, s + 1)]
            pa[pl.ds(s * nb, 2 * nb), pl.ds(LANES, LANES)] = jnp.concatenate(pair, axis=0).astype(BF16)

    ones_row = (iota((LANES, qtok), 0) == 0).astype(BF16)

    def score(block):
        rhs = jnp.concatenate([qb[block], ones_row], axis=0)
        half = dlen // 2
        best = [jnp.max(jnp.dot(pa[pl.ds(k * half * nb, half * nb)], rhs, preferred_element_type=F32)
                        .reshape(half, nb, qtok), axis=0) for k in range(2)]
        bm[block] = jnp.maximum(best[0], best[1])

    both = (to_y, to_core)
    arrive(bid(z, oy, c), (to_core,))
    arrive(bid(zx[0], y, c), both)
    score(me)
    arrive(bid(z, y, oc))
    score(bid(z, y, oc))
    score(bid(z, oy, c))
    score(bid(zx[0], y, c))
    arrive(bid(z, oy, oc))
    score(bid(z, oy, oc))
    arrive(bid(zx[0], oy, c), (to_core,))
    arrive(bid(zx[0], y, oc))
    score(bid(zx[0], y, oc))
    arrive(bid(zx[1], y, c), both)
    score(bid(zx[0], oy, c))
    score(bid(zx[1], y, c))
    arrive(bid(zx[0], oy, oc))
    score(bid(zx[0], oy, oc))
    arrive(bid(zx[1], y, oc))
    arrive(bid(zx[2], y, c), both)
    score(bid(zx[1], y, oc))
    arrive(bid(zx[1], oy, c), (to_core,))
    score(bid(zx[2], y, c))
    score(bid(zx[1], oy, c))
    arrive(bid(zx[2], y, oc))
    score(bid(zx[2], y, oc))
    arrive(bid(zx[1], oy, oc))
    arrive(bid(zx[2], oy, c), (to_core,))
    score(bid(zx[1], oy, oc))
    score(bid(zx[2], oy, c))
    arrive(bid(zx[2], oy, oc))
    score(bid(zx[2], oy, oc))

    best = bm[...].reshape(group * nb, qtok)
    sel = (iota((qtok, LANES), 0) // qlen == iota((qtok, LANES), 1) % nb).astype(BF16)
    hi = best.astype(BF16)
    rest = best - hi.astype(F32)
    mid = rest.astype(BF16)
    low = (rest - mid.astype(F32)).astype(BF16)
    tot = (jnp.dot(low, sel, preferred_element_type=F32)
           + jnp.dot(mid, sel, preferred_element_type=F32)
           + jnp.dot(hi, sel, preferred_element_type=F32))
    tot = tot.reshape(group, nb, LANES)
    here = iota((group, nb, LANES), 2) // nb == iota((group, nb, LANES), 0)
    scores = jnp.sum(jnp.where(here, tot, 0.0), axis=0)

    loads[4].wait()
    logits = scores / temp[0]
    top = jnp.max(logits, axis=0, keepdims=True)
    part = jnp.sum(jnp.exp(logits - top), axis=0, keepdims=True)
    mine = iota((nb, LANES), 1) == me * nb + iota((nb, LANES), 0)
    diag = jnp.sum(jnp.where(mine, logits, 0.0), axis=0, keepdims=True)
    st[me] = jnp.concatenate([top, part, diag, jnp.zeros_like(diag)], axis=0)

    stats = []
    for k in range(1, group):
        peer = (me + k) % group
        cp = pltpu.make_async_remote_copy(
            src_ref=st.at[me], dst_ref=st.at[me], send_sem=ssend_sem.at[k],
            recv_sem=srecv_sem.at[me],
            device_id={'data2': peer // (2 * ny), 'data': peer % (2 * ny)},
            device_id_type=pl.DeviceIdType.MESH)
        cp.start()
        stats.append(cp)
    for k in range(1, group):
        peer = (me + k) % group
        pltpu.make_async_remote_copy(
            src_ref=st.at[peer], dst_ref=st.at[peer], send_sem=ssend_sem.at[0],
            recv_sem=srecv_sem.at[peer], device_id=dev(z, y, oc),
            device_id_type=pl.DeviceIdType.MESH).wait_recv()

    tops = st[:, 0, :]
    best_top = jnp.max(tops, axis=0, keepdims=True)
    total = jnp.sum(st[:, 1, :] * jnp.exp(tops - best_top), axis=0, keepdims=True)
    losses = best_top + jnp.log(total) - jnp.sum(st[:, 2, :], axis=0, keepdims=True)
    mean = jnp.sum(losses, axis=1, keepdims=True) / (group * nb)
    moved = pltpu.roll(jnp.broadcast_to(losses, (8, LANES)), (LANES - me * nb) % LANES, 1)
    out_ref[...] = jnp.where(iota((1, LANES), 1) < nb, moved[0:1], mean)
    for cp in sends:
        cp.wait_send()
    for cp in stats:
        cp.wait_send()


def solution(mesh):
    nz, nd = mesh.shape['data2'], mesh.shape['data']
    ny = nd // 2
    group = nz * nd
    row_spec = P(('replica', 'data2', 'data'))
    tok_spec = P(('replica', 'data2', 'data'), None, None)
    mask_spec = P(('replica', 'data2', 'data'), None)

    def local_step(qh, dh, w, qm, dm, temp):
        nb, qlen, hidden = qh.shape
        dlen = dh.shape[1]
        parts = 6
        halves = 1
        dims = (nz, ny, nb, qlen, dlen, parts, halves, hidden)
        flat = jnp.transpose(dh, (1, 0, 2)).reshape(dlen * nb, hidden)
        out = pl.pallas_call(
            functools.partial(kernel, dims),
            out_shape=pltpu.VMEM((1, LANES), F32),
            in_specs=[pl.BlockSpec(memory_space=pl.ANY)] * 6,
            out_specs=pl.BlockSpec(memory_space=pltpu.VMEM),
            scratch_shapes=[
                pltpu.VMEM((nb, qlen, hidden), BF16),
                pltpu.VMEM((dlen * nb, hidden), BF16),
                pltpu.VMEM(w.shape, BF16),
                pltpu.VMEM((nb, qlen), jnp.int32),
                pltpu.VMEM((nb, dlen), jnp.int32),
                pltpu.SMEM((1,), F32),
                pltpu.VMEM((dlen * nb, 2 * LANES), BF16),
                pltpu.VMEM((group, LANES, nb * qlen), BF16),
                pltpu.VMEM((group, nb, nb * qlen), F32),
                pltpu.VMEM((group, 4, LANES), F32),
                pltpu.SemaphoreType.DMA((5,)),
                pltpu.SemaphoreType.DMA((parts,)),
                pltpu.SemaphoreType.DMA((group * halves,)),
                pltpu.SemaphoreType.DMA((group, halves)),
                pltpu.SemaphoreType.DMA((group,)),
                pltpu.SemaphoreType.DMA((group,)),
            ],
            compiler_params=pltpu.CompilerParams(collective_id=0, has_side_effects=True),
            name='late_interaction',
        )(qh, flat, w, qm, dm, temp.reshape(1))
        return out[0, :nb], out[0, nb:nb + 1]

    return jax.shard_map(
        local_step, mesh=mesh,
        in_specs=(tok_spec, tok_spec, P(None, None), mask_spec, mask_spec, P()),
        out_specs=(row_spec, P('replica')), check_vma=False)
```
